128 devices in a mesh: pair: 8 (over x_hi, y), aux: 16 (over x_lo, z, core).
Axes of the slice: x: 4 (x_hi: 2, x_lo: 2; x = x_hi * 2 + x_lo), y: 4, z: 4, core: 2. Of those that a mesh axis runs over, the one named last changes fastest.
Arguments:
- same_panels: bfloat16 [64, 2, 112, 59904], P('aux', None, None, 'pair'), may hold values from -1 to 1
- opposite_panels: bfloat16 [64, 2, 112, 59904], P('aux', None, None, 'pair'), may hold values from -1 to 1
- same_amplitudes: bfloat16 [64, 112, 112], replicated, may hold values from -2 to 2
- opposite_amplitudes: bfloat16 [64, 112, 112], replicated, may hold values from -2 to 2
- same_energies: float32 [64, 2, 112], replicated, may hold values from 0.5 to 3
- opposite_energies: float32 [64, 2, 112], replicated, may hold values from 0.5 to 3
- same_ranks: int32 [64], replicated, may hold values from 48 to 112
- opposite_ranks: int32 [64], replicated, may hold values from 48 to 112
Outputs:
- same_residual: float32 [64, 112, 112], P('pair', 'aux')
- opposite_residual: float32 [64, 112, 112], P('pair', 'aux')
The draws below stay inside these ranges and needn't reach their ends.
Inputs may be any that keep to these rules, and one draw needn't show every extreme that they name: `same_ranks`: slots at or beyond a pair's rank are padding. `opposite_ranks`: slots at or beyond a pair's rank are padding.
All inputs are finite; a program needn't handle non-finite values.
Results may differ from the reference program's by a relative error of at most 0.0013.
Values may be sent and summed in bfloat16 or wider, within the bound.
A program may use at most 128 MiB of HBM per device.

```python
import math
import jax
import jax.numpy as jnp
from jax import lax

R = 112
NAUX = 59904
PAIRS = 64


def with_ends(entries, key, least, top_value):
    dims = entries.shape
    index_at = [jax.random.randint(jax.random.fold_in(key, axis), (), 0, dims[axis]) for axis in range(len(dims))]
    entries = entries.at[tuple(index_at)].set(least)
    longest = dims.index(max(dims))
    index_at[longest] = (index_at[longest] + 1) % dims[longest]
    return entries.at[tuple(index_at)].set(top_value)


def steps_of(own_key, extent, shards, smallest, largest):
    def one(position, parts):
        heights = jax.random.uniform(jax.random.fold_in(jax.random.fold_in(own_key, 6), position), (parts,), jnp.float32, smallest / len(shards), largest / len(shards))
        return jnp.repeat(jnp.exp(heights), extent[position] // parts).reshape((-1,) + (1,) * (len(extent) - position - 1))

    level = one(*shards[0])
    for cut in shards[1:]:
        level = level * one(*cut)
    return level


def bell_draw(stream_key, shape, deviation, limit, pieces=(), kind=jnp.bfloat16):
    factor_of = steps_of(stream_key, shape, pieces, -0.22, 0.18) if pieces else 1.0
    values = jax.random.normal(stream_key, shape, jnp.float32) * deviation * factor_of
    return jnp.minimum(jnp.maximum(values, -limit), limit).astype(kind)


def setup_inputs(seed: int = 0) -> dict:
    arg_keys = jax.random.split(jax.random.key(seed), 9)
    same_panels = bell_draw(arg_keys[0], (PAIRS, 2, R, NAUX), (NAUX ** -0.25), 1.0, ((0, 16), (3, 8)))
    opposite_panels = bell_draw(arg_keys[1], (PAIRS, 2, R, NAUX), (NAUX ** -0.25), 1.0, ((0, 16), (3, 8)))
    same_amplitudes = bell_draw(arg_keys[2], (PAIRS, R, R), 0.15, 2.0)
    opposite_amplitudes = bell_draw(arg_keys[3], (PAIRS, R, R), 0.15, 2.0)
    same_energies = jnp.clip(jnp.exp(jax.random.uniform(arg_keys[4], (PAIRS, 2, R), jnp.float32, math.log(0.5), math.log(3.0))), 0.5, 3.0)
    opposite_energies = jnp.clip(jnp.exp(jax.random.uniform(arg_keys[5], (PAIRS, 2, R), jnp.float32, math.log(0.5), math.log(3.0))), 0.5, 3.0)
    same_ranks = with_ends(jax.random.randint(arg_keys[6], (PAIRS,), R * 3 // 7, R + 1), jax.random.fold_in(arg_keys[6], 1), R * 3 // 7, R).astype(jnp.int32)
    opposite_ranks = with_ends(jax.random.randint(arg_keys[7], (PAIRS,), R * 3 // 7, R + 1), jax.random.fold_in(arg_keys[7], 1), R * 3 // 7, R).astype(jnp.int32)
    return dict(same_panels=same_panels, opposite_panels=opposite_panels, same_amplitudes=same_amplitudes, opposite_amplitudes=opposite_amplitudes, same_energies=same_energies, opposite_energies=opposite_energies, same_ranks=same_ranks, opposite_ranks=opposite_ranks)


def slot_mask(ranks):
    slots = jnp.arange(R, dtype=jnp.int32)
    return (slots[None, :] < ranks[:, None]).astype(jnp.float32)


def masked_amplitudes(amplitudes, keep):
    outer = keep[:, :, None] * keep[:, None, :]
    return (amplitudes.astype(jnp.float32) * outer).astype(jnp.bfloat16)


def dressing_rows(panels, masked):
    def one_pair(items):
        panel, amplitude = items
        mixed = jnp.dot(amplitude, panel[1], preferred_element_type=jnp.float32)
        return jnp.sum(panel[0].astype(jnp.float32) * mixed, axis=0)
    return lax.map(one_pair, (panels, masked))


def residual_rows(panels, masked, energies, keep, coupling):
    def one_pair(items):
        panel, amplitude, energy, mask_row = items
        exchange = jnp.dot(panel[0], panel[1].T, preferred_element_type=jnp.float32)
        scaled = (panel[0].astype(jnp.float32) * coupling[None, :]).astype(jnp.bfloat16)
        coulomb = jnp.dot(scaled, panel[1].T, preferred_element_type=jnp.float32)
        diagonal = (energy[0][:, None] + energy[1][None, :]) * amplitude.astype(jnp.float32)
        return (exchange + coulomb + diagonal) * (mask_row[:, None] * mask_row[None, :])
    return lax.map(one_pair, (panels, masked, energies, keep))


def reference(same_panels, opposite_panels, same_amplitudes, opposite_amplitudes, same_energies, opposite_energies, same_ranks, opposite_ranks):
    same_keep = slot_mask(same_ranks)
    opposite_keep = slot_mask(opposite_ranks)
    same_masked = masked_amplitudes(same_amplitudes, same_keep)
    opposite_masked = masked_amplitudes(opposite_amplitudes, opposite_keep)
    coupling = jnp.sum(dressing_rows(same_panels, same_masked), axis=0) + jnp.sum(dressing_rows(opposite_panels, opposite_masked), axis=0)
    same_residual = residual_rows(same_panels, same_masked, same_energies, same_keep, coupling)
    opposite_residual = residual_rows(opposite_panels, opposite_masked, opposite_energies, opposite_keep, coupling)
    return same_residual, opposite_residual
```

```python
import jax
import jax.numpy as jnp
from jax import lax
from jax.experimental import pallas as pl
from jax.experimental.pallas import tpu as pltpu
from jax.sharding import PartitionSpec as P

f32 = jnp.float32
bf16 = jnp.bfloat16
MESH = pl.DeviceIdType.MESH

R = 112
CHUNKS = ((0, 2048), (2048, 2048), (4096, 2048), (6144, 1344))
BLOCK = 1024
NT = (((1,), (1,)), ((), ()))


def tiles_of(width):
    return (width + 127) // 128


def kernel(
    sp, op, sa, oa, se, oe, sr, orr, out_s, out_o,
    pan0, pan1, pan2, pan3,
    raw, tm, famp, fen, fadd, fmask,
    cp0, cp1, cp2, cp3, cr0, cr1, cr2, cr3, cs,
    acc, sb1, rb1, sb2, rb2,
    pan_sem, raw_sem, fin_sem, c_send, c_recv, s1_send, s1_recv, s2_send, s2_recv,
):
    p = lax.axis_index("pair")
    a = lax.axis_index("aux")
    pan = (pan0, pan1, pan2, pan3)
    cps = (cp0, cp1, cp2, cp3)
    crs = (cr0, cr1, cr2, cr3)
    diagonal = p == a // 2

    raw_copies = [
        pltpu.make_async_copy(src.at[pl.ds(4 * a, 4)], raw.at[pl.ds(4 * s, 4)], raw_sem.at[s])
        for s, src in enumerate((sa, oa))
    ]
    for copy in raw_copies:
        copy.start()
    pan_copies = []
    for c, (start, width) in enumerate(CHUNKS):
        row = []
        for i in range(8):
            src = (sp if i < 4 else op).at[i % 4, :, :, pl.ds(start, width)]
            copy = pltpu.make_async_copy(src, pan[c].at[i], pan_sem.at[c, i])
            copy.start()
            row.append(copy)
        pan_copies.append(row)
    fin_copies = []
    for s, (amp, en) in enumerate(((sa, se), (oa, oe))):
        fin_copies.append(
            pltpu.make_async_copy(amp.at[pl.ds(8 * p, 8)], famp.at[pl.ds(8 * s, 8)], fin_sem.at[s])
        )
        fin_copies.append(
            pltpu.make_async_copy(en.at[pl.ds(8 * p, 8)], fen.at[pl.ds(8 * s, 8)], fin_sem.at[2 + s])
        )
    for copy in fin_copies:
        copy.start()

    barrier = pltpu.get_barrier_semaphore()
    for k in range(1, 16):
        pl.semaphore_signal(
            barrier, inc=1, device_id=(p, lax.rem(a + k, 16)), device_id_type=MESH
        )
    for k in range(1, 8):
        pl.semaphore_signal(barrier, inc=1, device_id=(lax.rem(p + k, 8), a), device_id_type=MESH)
    own = lax.rem(a, 2)
    for k in range(2):

        @pl.when(jnp.logical_not(jnp.logical_and(diagonal, own == k)))
        def _():
            pl.semaphore_signal(
                barrier, inc=1, device_id=(a // 2, 2 * p + k), device_id_type=MESH
            )

    for copy in raw_copies:
        copy.wait()
    rows_i = lax.broadcasted_iota(jnp.int32, (R, R), 0)
    cols_i = lax.broadcasted_iota(jnp.int32, (R, R), 1)
    for i in range(8):
        rank = (sr if i < 4 else orr)[4 * a + i % 4]
        kept = jnp.logical_and(rows_i < rank, cols_i < rank)
        tm[i] = jnp.where(kept, raw[i].astype(f32), 0.0).astype(bf16)

    def mixed(c):
        width = CHUNKS[c][1]

        def block(tile, offset, size):
            total = jnp.zeros((8, size), f32)
            for i in range(8):
                m = jnp.dot(
                    tm[i], pan[c][i, 1, :, pl.ds(offset, size)], preferred_element_type=f32
                )
                prod = m * pan[c][i, 0, :, pl.ds(offset, size)].astype(f32)
                total = total + jnp.sum(prod.reshape(14, 8, size), axis=0)
            line = jnp.sum(total, axis=0, keepdims=True)
            for k in range(tiles_of(size)):
                part = min(128, size - 128 * k)
                cps[c][pl.ds(tile + k, 1), 0:part] = line[:, 128 * k : 128 * k + part]

        full = width // BLOCK

        def step(n, carry):
            block(n * (BLOCK // 128), pl.multiple_of(n * BLOCK, BLOCK), BLOCK)
            return carry

        lax.fori_loop(0, full, step, 0)
        if width > full * BLOCK:
            block(full * (BLOCK // 128), full * BLOCK, width - full * BLOCK)

    def send_coupling(c):
        for k in range(1, 16):
            pltpu.make_async_remote_copy(
                src_ref=cps[c],
                dst_ref=crs[c].at[k - 1],
                send_sem=c_send.at[c],
                recv_sem=c_recv.at[c],
                device_id=(p, lax.rem(a + k, 16)),
                device_id_type=MESH,
            ).start()

    def take_coupling(c):
        pltpu.make_async_copy(crs[c], crs[c], c_recv.at[c]).wait()
        total = cps[c][...]
        for k in range(15):
            total = total + crs[c][k]
        cs[c] = total

    def exchange(c):
        for i in range(8):
            e = lax.dot_general(pan[c][i, 0], pan[c][i, 1], NT, preferred_element_type=f32)
            acc[i] = e if c == 0 else acc[i] + e

    def coulomb(c, i):
        width = CHUNKS[c][1]
        parts = []
        for t in range(tiles_of(width)):
            size = min(128, width - 128 * t)
            left = pan[c][i, 0, :, 128 * t : 128 * t + size].astype(f32)
            parts.append((left * cs[c, t : t + 1, 0:size]).astype(bf16))
        scaled = jnp.concatenate(parts, axis=1)
        return lax.dot_general(scaled, pan[c][i, 1], NT, preferred_element_type=f32)

    for c in range(4):
        cps[c][...] = jnp.zeros_like(cps[c])
        for i in range(8):
            pan_copies[c][i].wait()
        mixed(c)
        if c == 0:
            pl.semaphore_wait(barrier, 24 - diagonal.astype(jnp.int32))
        send_coupling(c)
        exchange(c)

    for c in range(3):
        take_coupling(c)
        for i in range(8):
            acc[i] = acc[i] + coulomb(c, i)

    for copy in fin_copies:
        copy.wait()
    sel_r = lax.broadcasted_iota(jnp.int32, (16, R), 0)
    sel_c = lax.broadcasted_iota(jnp.int32, (16, R), 1)
    first = 7 * a
    chosen = jnp.logical_and(sel_c == first + sel_r, sel_r < 7)
    select = chosen.astype(f32).astype(bf16)
    pick = chosen[0:8].astype(f32)
    for k in range(16):
        rank = (sr if k < 8 else orr)[8 * p + k % 8]
        amp = jnp.dot(select, famp[k], preferred_element_type=f32)[0:8]
        first_gap = jnp.sum(pick * fen[k, 0:1, :], axis=1, keepdims=True)
        kept = jnp.logical_and(first + sel_r[0:8] < rank, sel_c[0:8] < rank)
        fmask[k] = kept.astype(f32)
        fadd[k] = (first_gap + fen[k, 1:2, :]) * amp

    take_coupling(3)
    for s in range(2):
        for j in range(4):
            i = 4 * s + j
            total = acc[i] + coulomb(3, i)
            for d in range(8):
                sb1[d, s, 14 * j : 14 * j + 14, 0:R] = total[14 * d : 14 * d + 14]
        for k in range(1, 8):
            d = lax.rem(p + k, 8)
            pltpu.make_async_remote_copy(
                src_ref=sb1.at[d, s],
                dst_ref=rb1.at[s, k - 1],
                send_sem=s1_send.at[s],
                recv_sem=s1_recv.at[s],
                device_id=(d, a),
                device_id_type=MESH,
            ).start()

    for s in range(2):
        pltpu.make_async_copy(rb1.at[s], rb1.at[s], s1_recv.at[s]).wait()
        total = sb1[p, s]
        for k in range(7):
            total = total + rb1[s, k]
        for j in range(4):
            for q in range(2):
                sb2[q, s, j, 0:7, :] = total[14 * j + 7 * q : 14 * j + 7 * q + 7]
        for q in range(2):
            mine = jnp.logical_and(diagonal, own == q)

            @pl.when(mine)
            def _():
                rb2[q, s] = sb2[q, s]

            @pl.when(jnp.logical_not(mine))
            def _():
                pltpu.make_async_remote_copy(
                    src_ref=sb2.at[q, s],
                    dst_ref=rb2.at[own, s],
                    send_sem=s2_send.at[q, s],
                    recv_sem=s2_recv.at[own, s],
                    device_id=(a // 2, 2 * p + q),
                    device_id_type=MESH,
                ).start()

    for s, out in enumerate((out_s, out_o)):
        for b in range(2):

            @pl.when(jnp.logical_not(jnp.logical_and(diagonal, own == b)))
            def _():
                pltpu.make_async_copy(rb2.at[b, s], rb2.at[b, s], s2_recv.at[b, s]).wait()
                pltpu.make_async_copy(rb2.at[b, s], rb2.at[b, s], s2_send.at[b, s]).wait()

            for j in range(4):
                k = 8 * s + 4 * b + j
                value = (rb2[b, s, j, :, 0:R] + fadd[k]) * fmask[k]
                out[4 * b + j] = value[0:7]

    for c in range(4):
        pltpu.make_async_copy(crs[c], crs[c], c_send.at[c]).wait()
    for s in range(2):
        pltpu.make_async_copy(rb1.at[s], rb1.at[s], s1_send.at[s]).wait()


def body(sp, op, sa, oa, se, oe, sr, orr):
    any_space = pl.BlockSpec(memory_space=pl.ANY)
    smem = pl.BlockSpec(memory_space=pltpu.SMEM)
    vmem = pl.BlockSpec(memory_space=pltpu.VMEM)
    out = jax.ShapeDtypeStruct((8, 7, R), f32)
    rows = 16
    sem = pltpu.SemaphoreType.DMA
    return pl.pallas_call(
        kernel,
        out_shape=[out, out],
        in_specs=[any_space] * 6 + [smem] * 2,
        out_specs=[vmem, vmem],
        scratch_shapes=[pltpu.VMEM((8, 2, R, w), bf16) for _, w in CHUNKS]
        + [
            pltpu.VMEM((8, R, R), bf16),
            pltpu.VMEM((8, R, R), bf16),
            pltpu.VMEM((16, R, R), bf16),
            pltpu.VMEM((16, 2, R), f32),
            pltpu.VMEM((16, 8, R), f32),
            pltpu.VMEM((16, 8, R), f32),
        ]
        + [pltpu.VMEM((rows, 128), f32)] * 4
        + [pltpu.VMEM((15, rows, 128), f32)] * 4
        + [
            pltpu.VMEM((4, rows, 128), f32),
            pltpu.VMEM((8, R, R), f32),
            pltpu.VMEM((8, 2, 56, 128), f32),
            pltpu.VMEM((2, 7, 56, 128), f32),
            pltpu.VMEM((2, 2, 4, 8, 128), f32),
            pltpu.VMEM((2, 2, 4, 8, 128), f32),
            sem((4, 8)),
            sem((2,)),
            sem((4,)),
            sem((4,)),
            sem((4,)),
            sem((2,)),
            sem((2,)),
            sem((2, 2)),
            sem((2, 2)),
        ],
        compiler_params=pltpu.CompilerParams(
            collective_id=0, has_side_effects=True, vmem_limit_bytes=60 * 1024 * 1024
        ),
    )(sp, op, sa, oa, se, oe, sr, orr)


def solution(mesh):
    panels = P("aux", None, None, "pair")
    return jax.shard_map(
        body,
        mesh=mesh,
        in_specs=(panels, panels) + (P(),) * 6,
        out_specs=(P("pair", "aux", None), P("pair", "aux", None)),
        check_vma=False,
    )
```

```python
import jax
import jax.numpy as jnp
from jax import lax
from jax.experimental import pallas as pl
from jax.experimental.pallas import tpu as pltpu
from jax.sharding import PartitionSpec as P

f32 = jnp.float32
bf16 = jnp.bfloat16
MESH = pl.DeviceIdType.MESH

R = 112
CHUNKS = ((0, 1024), (1024, 2048), (3072, 2304), (5376, 2112))
N = len(CHUNKS)
NT = (((1,), (1,)), ((), ()))


def tiles_of(width):
    return (width + 127) // 128


def rows_of(width):
    return (tiles_of(width) + 7) // 8 * 8


def kernel(
    sp, op, sa, oa, se, oe, sr, orr, out_s, out_o, *scratch
):
    pan, cps, crs, cs = (scratch[N * k : N * k + N] for k in range(4))
    (
        raw, tm, famp, fen, fadd, fmask, acc, tot, sb1, rb1, sb2, rb2,
        pan_sem, raw_sem, fin_sem, c_send, c_recv, s1_send, s1_recv, s2_send, s2_recv,
    ) = scratch[4 * N :]
    p = lax.axis_index("pair")
    a = lax.axis_index("aux")
    diagonal = p == a // 2

    raw_copies = [
        pltpu.make_async_copy(src.at[pl.ds(4 * a, 4)], raw.at[pl.ds(4 * s, 4)], raw_sem.at[s])
        for s, src in enumerate((sa, oa))
    ]
    for copy in raw_copies:
        copy.start()
    pan_copies = []
    for c, (start, width) in enumerate(CHUNKS):
        row = []
        for i in range(8):
            src = (sp if i < 4 else op).at[i % 4, :, :, pl.ds(start, width)]
            copy = pltpu.make_async_copy(src, pan[c].at[i], pan_sem.at[c, i])
            copy.start(priority=1)
            row.append(copy)
        pan_copies.append(row)
    fin_copies = []
    for s, (amp, en) in enumerate(((sa, se), (oa, oe))):
        fin_copies.append(
            pltpu.make_async_copy(amp.at[pl.ds(8 * p, 8)], famp.at[pl.ds(8 * s, 8)], fin_sem.at[s])
        )
        fin_copies.append(
            pltpu.make_async_copy(en.at[pl.ds(8 * p, 8)], fen.at[pl.ds(8 * s, 8)], fin_sem.at[2 + s])
        )
    for copy in fin_copies:
        copy.start()

    barrier = pltpu.get_barrier_semaphore()
    for k in range(1, 16):
        pl.semaphore_signal(
            barrier, inc=1, device_id=(p, lax.rem(a + k, 16)), device_id_type=MESH
        )
    for k in range(1, 8):
        pl.semaphore_signal(barrier, inc=1, device_id=(lax.rem(p + k, 8), a), device_id_type=MESH)
    own = lax.rem(a, 2)
    for k in range(2):

        @pl.when(jnp.logical_not(jnp.logical_and(diagonal, own == k)))
        def _():
            pl.semaphore_signal(
                barrier, inc=1, device_id=(a // 2, 2 * p + k), device_id_type=MESH
            )

    for copy in raw_copies:
        copy.wait()
    rows_i = lax.broadcasted_iota(jnp.int32, (R, R), 0)
    cols_i = lax.broadcasted_iota(jnp.int32, (R, R), 1)
    for i in range(8):
        rank = (sr if i < 4 else orr)[4 * a + i % 4]
        kept = jnp.logical_and(rows_i < rank, cols_i < rank)
        tm[i] = jnp.where(kept, raw[i].astype(f32), 0.0).astype(bf16)

    def mixed(c):
        width = CHUNKS[c][1]

        total = jnp.zeros((8, width), f32)
        for i in range(8):
            m = jnp.dot(tm[i], pan[c][i, 1], preferred_element_type=f32)
            prod = m * pan[c][i, 0].astype(f32)
            total = total + jnp.sum(prod.reshape(14, 8, width), axis=0)
        line = jnp.sum(total, axis=0, keepdims=True)
        for k in range(tiles_of(width)):
            part = min(128, width - 128 * k)
            cps[c][k : k + 1, 0:part] = line[:, 128 * k : 128 * k + part]

    def send_coupling(c):
        for k in range(1, 16):
            pltpu.make_async_remote_copy(
                src_ref=cps[c],
                dst_ref=crs[c].at[k - 1],
                send_sem=c_send.at[c],
                recv_sem=c_recv.at[c],
                device_id=(p, lax.rem(a + k, 16)),
                device_id_type=MESH,
            ).start()

    def take_coupling(c):
        pltpu.make_async_copy(crs[c], crs[c], c_recv.at[c]).wait()
        total = cps[c][...]
        for k in range(15):
            total = total + crs[c][k]
        cs[c][...] = total

    def exchange(c):
        for i in range(8):
            e = lax.dot_general(pan[c][i, 0], pan[c][i, 1], NT, preferred_element_type=f32)
            acc[i] = e if c == 0 else acc[i] + e

    def coulomb(c, i):
        width = CHUNKS[c][1]
        parts = []
        for t in range(tiles_of(width)):
            size = min(128, width - 128 * t)
            left = pan[c][i, 0, :, 128 * t : 128 * t + size].astype(f32)
            parts.append((left * cs[c][t : t + 1, 0:size]).astype(bf16))
        scaled = jnp.concatenate(parts, axis=1)
        return lax.dot_general(scaled, pan[c][i, 1], NT, preferred_element_type=f32)

    tot[...] = jnp.zeros_like(tot)
    for c in range(N):
        cps[c][...] = jnp.zeros_like(cps[c])
        for i in range(8):
            pan_copies[c][i].wait()
        mixed(c)
        if c == 0:
            pl.semaphore_wait(barrier, 24 - diagonal.astype(jnp.int32))
        send_coupling(c)
        exchange(c)

    for c in range(N - 1):
        take_coupling(c)
        for i in range(8):
            acc[i] = acc[i] + coulomb(c, i)

    for copy in fin_copies:
        copy.wait()
    sel_r = lax.broadcasted_iota(jnp.int32, (16, R), 0)
    sel_c = lax.broadcasted_iota(jnp.int32, (16, R), 1)
    first = 7 * a
    chosen = jnp.logical_and(sel_c == first + sel_r, sel_r < 7)
    select = chosen.astype(f32).astype(bf16)
    pick = chosen[0:8].astype(f32)
    for k in range(16):
        rank = (sr if k < 8 else orr)[8 * p + k % 8]
        amp = jnp.dot(select, famp[k], preferred_element_type=f32)[0:8]
        first_gap = jnp.sum(pick * fen[k, 0:1, :], axis=1, keepdims=True)
        kept = jnp.logical_and(first + sel_r[0:8] < rank, sel_c[0:8] < rank).astype(f32)
        added = (first_gap + fen[k, 1:2, :]) * amp
        for r in range(7):
            fmask[k // 8, r, k % 8 : k % 8 + 1, :] = kept[r : r + 1]
            fadd[k // 8, r, k % 8 : k % 8 + 1, :] = added[r : r + 1]

    take_coupling(N - 1)
    for s in range(2):
        for j in range(4):
            i = 4 * s + j
            total = acc[i] + coulomb(N - 1, i)
            tot[i, :, 0:R] = total
            for d in range(8):
                sb1[d, s, pl.ds(j, 14, stride=4), :] = tot[i, 14 * d : 14 * d + 14, :]
        for k in range(1, 8):
            d = lax.rem(p + k, 8)
            pltpu.make_async_remote_copy(
                src_ref=sb1.at[d, s],
                dst_ref=rb1.at[s, k - 1],
                send_sem=s1_send.at[s],
                recv_sem=s1_recv.at[s],
                device_id=(d, a),
                device_id_type=MESH,
            ).start()

    for s in range(2):
        pltpu.make_async_copy(rb1.at[s], rb1.at[s], s1_recv.at[s]).wait()
        total = sb1[p, s]
        for k in range(7):
            total = total + rb1[s, k]
        for r in range(14):
            sb2[r // 7, s, r % 7] = total[4 * r : 4 * r + 4]
        for q in range(2):
            mine = jnp.logical_and(diagonal, own == q)

            @pl.when(mine)
            def _():
                rb2[q, s] = sb2[q, s]

            @pl.when(jnp.logical_not(mine))
            def _():
                pltpu.make_async_remote_copy(
                    src_ref=sb2.at[q, s],
                    dst_ref=rb2.at[own, s],
                    send_sem=s2_send.at[q, s],
                    recv_sem=s2_recv.at[own, s],
                    device_id=(a // 2, 2 * p + q),
                    device_id_type=MESH,
                ).start()

    for s, out in enumerate((out_s, out_o)):
        for b in range(2):

            @pl.when(jnp.logical_not(jnp.logical_and(diagonal, own == b)))
            def _():
                pltpu.make_async_copy(rb2.at[b, s], rb2.at[b, s], s2_recv.at[b, s]).wait()
                pltpu.make_async_copy(rb2.at[b, s], rb2.at[b, s], s2_send.at[b, s]).wait()

        for r in range(7):
            value = jnp.concatenate([rb2[0, s, r, :, 0:R], rb2[1, s, r, :, 0:R]], axis=0)
            out[r] = (value + fadd[s, r]) * fmask[s, r]

    for c in range(N):
        pltpu.make_async_copy(crs[c], crs[c], c_send.at[c]).wait()
    for s in range(2):
        pltpu.make_async_copy(rb1.at[s], rb1.at[s], s1_send.at[s]).wait()


def hand_out(same, opposite, out_s, out_o):
    out_s[...] = same[...]
    out_o[...] = opposite[...]


def body(sp, op, sa, oa, se, oe, sr, orr):
    any_space = pl.BlockSpec(memory_space=pl.ANY)
    smem = pl.BlockSpec(memory_space=pltpu.SMEM)
    vmem = pl.BlockSpec(memory_space=pltpu.VMEM)
    out = jax.ShapeDtypeStruct((7, 8, R), f32)
    sem = pltpu.SemaphoreType.DMA
    same, opposite = pl.pallas_call(
        kernel,
        out_shape=[out, out],
        in_specs=[any_space] * 6 + [smem] * 2,
        out_specs=[vmem, vmem],
        scratch_shapes=[pltpu.VMEM((8, 2, R, w), bf16) for _, w in CHUNKS]
        + [pltpu.VMEM((rows_of(w), 128), f32) for _, w in CHUNKS]
        + [pltpu.VMEM((15, rows_of(w), 128), f32) for _, w in CHUNKS]
        + [pltpu.VMEM((rows_of(w), 128), f32) for _, w in CHUNKS]
        + [
            pltpu.VMEM((8, R, R), bf16),
            pltpu.VMEM((8, R, R), bf16),
            pltpu.VMEM((16, R, R), bf16),
            pltpu.VMEM((16, 2, R), f32),
            pltpu.VMEM((2, 7, 8, R), f32),
            pltpu.VMEM((2, 7, 8, R), f32),
            pltpu.VMEM((8, R, R), f32),
            pltpu.VMEM((8, R, 128), f32),
            pltpu.VMEM((8, 2, 56, 128), f32),
            pltpu.VMEM((2, 7, 56, 128), f32),
            pltpu.VMEM((2, 2, 7, 4, 128), f32),
            pltpu.VMEM((2, 2, 7, 4, 128), f32),
            sem((N, 8)),
            sem((2,)),
            sem((4,)),
            sem((N,)),
            sem((N,)),
            sem((2,)),
            sem((2,)),
            sem((2, 2)),
            sem((2, 2)),
        ],
        compiler_params=pltpu.CompilerParams(
            collective_id=0, has_side_effects=True, vmem_limit_bytes=60 * 1024 * 1024
        ),
    )(sp, op, sa, oa, se, oe, sr, orr)
    same, opposite = pl.pallas_call(
        hand_out,
        out_shape=[out, out],
        in_specs=[vmem, vmem],
        out_specs=[vmem, vmem],
    )(same, opposite)
    return jnp.transpose(same, (1, 0, 2)), jnp.transpose(opposite, (1, 0, 2))


def solution(mesh):
    panels = P("aux", None, None, "pair")
    return jax.shard_map(
        body,
        mesh=mesh,
        in_specs=(panels, panels) + (P(),) * 6,
        out_specs=(P("pair", "aux", None), P("pair", "aux", None)),
        check_vma=False,
    )
```

```python
import jax
import jax.numpy as jnp
from jax import lax
from jax.experimental import pallas as pl
from jax.experimental.pallas import tpu as pltpu
from jax.sharding import PartitionSpec as P

f32 = jnp.float32
bf16 = jnp.bfloat16
MESH = pl.DeviceIdType.MESH

R = 112
CHUNKS = ((0, 1024), (1024, 1792), (2816, 2048), (4864, 1664), (6528, 960))
N = len(CHUNKS)
HELD = 3
LATE = 4
NT = (((1,), (1,)), ((), ()))


def tiles_of(width):
    return (width + 127) // 128


def rows_of(width):
    return (tiles_of(width) + 7) // 8 * 8


def kernel(
    sp, op, sa, oa, se, oe, sr, orr, out_s, out_o, *scratch
):
    pan, cps, crs, cs = (scratch[N * k : N * k + N] for k in range(4))
    (
        raw, tm, famp, fen, fadd, fmask, acc, tot, sb1, rb1, sb2, rb2,
        pan_sem, raw_sem, fin_sem, c_send, c_recv, s1_send, s1_recv, s2_send, s2_recv,
    ) = scratch[4 * N :]
    p = lax.axis_index("pair")
    a = lax.axis_index("aux")
    diagonal = p == a // 2

    raw_copies = [
        pltpu.make_async_copy(src.at[pl.ds(4 * a, 4)], raw.at[pl.ds(4 * s, 4)], raw_sem.at[s])
        for s, src in enumerate((sa, oa))
    ]
    for copy in raw_copies:
        copy.start()
    pan_copies = []
    for c, (start, width) in enumerate(CHUNKS):
        row = []
        for i in range(8):
            src = (sp if i < 4 else op).at[i % 4, :, :, pl.ds(start, width)]
            copy = pltpu.make_async_copy(src, pan[c].at[i], pan_sem.at[c, i])
            copy.start(priority=1)
            row.append(copy)
        pan_copies.append(row)
    fin_copies = []
    for s, (amp, en) in enumerate(((sa, se), (oa, oe))):
        fin_copies.append(
            pltpu.make_async_copy(amp.at[pl.ds(8 * p, 8)], famp.at[pl.ds(8 * s, 8)], fin_sem.at[s])
        )
        fin_copies.append(
            pltpu.make_async_copy(en.at[pl.ds(8 * p, 8)], fen.at[pl.ds(8 * s, 8)], fin_sem.at[2 + s])
        )
    for copy in fin_copies:
        copy.start()

    barrier = pltpu.get_barrier_semaphore()
    for k in range(1, 16):
        pl.semaphore_signal(
            barrier, inc=1, device_id=(p, lax.rem(a + k, 16)), device_id_type=MESH
        )
    for k in range(1, 8):
        pl.semaphore_signal(barrier, inc=1, device_id=(lax.rem(p + k, 8), a), device_id_type=MESH)
    own = lax.rem(a, 2)
    for k in range(2):

        @pl.when(jnp.logical_not(jnp.logical_and(diagonal, own == k)))
        def _():
            pl.semaphore_signal(
                barrier, inc=1, device_id=(a // 2, 2 * p + k), device_id_type=MESH
            )

    for copy in raw_copies:
        copy.wait()
    rows_i = lax.broadcasted_iota(jnp.int32, (R, R), 0)
    cols_i = lax.broadcasted_iota(jnp.int32, (R, R), 1)
    for i in range(8):
        rank = (sr if i < 4 else orr)[4 * a + i % 4]
        kept = jnp.logical_and(rows_i < rank, cols_i < rank)
        tm[i] = jnp.where(kept, raw[i].astype(f32), 0.0).astype(bf16)

    def mixed(c):
        width = CHUNKS[c][1]

        total = jnp.zeros((8, width), f32)
        for i in range(8):
            m = jnp.dot(tm[i], pan[c][i, 1], preferred_element_type=f32)
            prod = m * pan[c][i, 0].astype(f32)
            total = total + jnp.sum(prod.reshape(14, 8, width), axis=0)
        line = jnp.sum(total, axis=0, keepdims=True)
        for k in range(tiles_of(width)):
            part = min(128, width - 128 * k)
            cps[c][k : k + 1, 0:part] = line[:, 128 * k : 128 * k + part]

    def send_coupling(c):
        for k in range(1, 16):
            pltpu.make_async_remote_copy(
                src_ref=cps[c],
                dst_ref=crs[c].at[k - 1],
                send_sem=c_send.at[c],
                recv_sem=c_recv.at[c],
                device_id=(p, lax.rem(a + k, 16)),
                device_id_type=MESH,
            ).start()

    def take_coupling(c):
        pltpu.make_async_copy(crs[c], crs[c], c_recv.at[c]).wait()
        total = cps[c][...]
        for k in range(15):
            total = total + crs[c][k]
        cs[c][...] = total

    def exchange(c):
        for i in range(8):
            e = lax.dot_general(pan[c][i, 0], pan[c][i, 1], NT, preferred_element_type=f32)
            acc[i] = e if c == 0 else acc[i] + e

    def coulomb(c, i):
        width = CHUNKS[c][1]
        parts = []
        for t in range(tiles_of(width)):
            size = min(128, width - 128 * t)
            left = pan[c][i, 0, :, 128 * t : 128 * t + size].astype(f32)
            parts.append((left * cs[c][t : t + 1, 0:size]).astype(bf16))
        scaled = jnp.concatenate(parts, axis=1)
        return lax.dot_general(scaled, pan[c][i, 1], NT, preferred_element_type=f32)

    tot[...] = jnp.zeros_like(tot)
    tot[...] = jnp.zeros_like(tot)

    def prepare(c):
        cps[c][...] = jnp.zeros_like(cps[c])
        for i in range(8):
            pan_copies[c][i].wait()
        mixed(c)
        if c == 0:
            pl.semaphore_wait(barrier, 24 - diagonal.astype(jnp.int32))
        send_coupling(c)

    for c in range(N):
        prepare(c)
        if c < N - HELD:
            exchange(c)
    for c in range(N - HELD, N):
        exchange(c)

    for c in range(N - LATE):
        take_coupling(c)
        for i in range(8):
            acc[i] = acc[i] + coulomb(c, i)

    for copy in fin_copies:
        copy.wait()
    sel_r = lax.broadcasted_iota(jnp.int32, (16, R), 0)
    sel_c = lax.broadcasted_iota(jnp.int32, (16, R), 1)
    first = 7 * a
    chosen = jnp.logical_and(sel_c == first + sel_r, sel_r < 7)
    select = chosen.astype(f32).astype(bf16)
    pick = chosen[0:8].astype(f32)
    for k in range(16):
        rank = (sr if k < 8 else orr)[8 * p + k % 8]
        amp = jnp.dot(select, famp[k], preferred_element_type=f32)[0:8]
        first_gap = jnp.sum(pick * fen[k, 0:1, :], axis=1, keepdims=True)
        kept = jnp.logical_and(first + sel_r[0:8] < rank, sel_c[0:8] < rank).astype(f32)
        added = (first_gap + fen[k, 1:2, :]) * amp
        for r in range(7):
            fmask[k // 8, r, k % 8 : k % 8 + 1, :] = kept[r : r + 1]
            fadd[k // 8, r, k % 8 : k % 8 + 1, :] = added[r : r + 1]

    for c in range(N - LATE, N):
        take_coupling(c)
    for s in range(2):
        for j in range(4):
            i = 4 * s + j
            total = acc[i]
            for c in range(N - LATE, N):
                total = total + coulomb(c, i)
            tot[i, :, 0:R] = total
            for d in range(8):
                sb1[d, s, pl.ds(j, 14, stride=4), :] = tot[i, 14 * d : 14 * d + 14, :]
        for k in range(1, 8):
            d = lax.rem(p + k, 8)
            pltpu.make_async_remote_copy(
                src_ref=sb1.at[d, s],
                dst_ref=rb1.at[s, k - 1],
                send_sem=s1_send.at[s],
                recv_sem=s1_recv.at[s],
                device_id=(d, a),
                device_id_type=MESH,
            ).start()

    for s in range(2):
        pltpu.make_async_copy(rb1.at[s], rb1.at[s], s1_recv.at[s]).wait()
        total = sb1[p, s]
        for k in range(7):
            total = total + rb1[s, k]
        for r in range(14):
            sb2[r // 7, s, r % 7] = total[4 * r : 4 * r + 4]
        for q in range(2):
            mine = jnp.logical_and(diagonal, own == q)

            @pl.when(mine)
            def _():
                rb2[q, s] = sb2[q, s]

            @pl.when(jnp.logical_not(mine))
            def _():
                pltpu.make_async_remote_copy(
                    src_ref=sb2.at[q, s],
                    dst_ref=rb2.at[own, s],
                    send_sem=s2_send.at[q, s],
                    recv_sem=s2_recv.at[own, s],
                    device_id=(a // 2, 2 * p + q),
                    device_id_type=MESH,
                ).start()

    for s, out in enumerate((out_s, out_o)):
        for b in range(2):

            @pl.when(jnp.logical_not(jnp.logical_and(diagonal, own == b)))
            def _():
                pltpu.make_async_copy(rb2.at[b, s], rb2.at[b, s], s2_recv.at[b, s]).wait()
                pltpu.make_async_copy(rb2.at[b, s], rb2.at[b, s], s2_send.at[b, s]).wait()

        for r in range(7):
            value = jnp.concatenate([rb2[0, s, r, :, 0:R], rb2[1, s, r, :, 0:R]], axis=0)
            out[r] = (value + fadd[s, r]) * fmask[s, r]

    for c in range(N):
        pltpu.make_async_copy(crs[c], crs[c], c_send.at[c]).wait()
    for s in range(2):
        pltpu.make_async_copy(rb1.at[s], rb1.at[s], s1_send.at[s]).wait()


def hand_out(same, opposite, out_s, out_o):
    out_s[...] = same[...]
    out_o[...] = opposite[...]


def body(sp, op, sa, oa, se, oe, sr, orr):
    any_space = pl.BlockSpec(memory_space=pl.ANY)
    smem = pl.BlockSpec(memory_space=pltpu.SMEM)
    vmem = pl.BlockSpec(memory_space=pltpu.VMEM)
    out = jax.ShapeDtypeStruct((7, 8, R), f32)
    sem = pltpu.SemaphoreType.DMA
    sp, op, sa, oa, se, oe, sr, orr = (
        pltpu.with_memory_space_constraint(x, pltpu.HBM) for x in (sp, op, sa, oa, se, oe, sr, orr)
    )
    same, opposite = pl.pallas_call(
        kernel,
        out_shape=[out, out],
        in_specs=[any_space] * 6 + [smem] * 2,
        out_specs=[vmem, vmem],
        scratch_shapes=[pltpu.VMEM((8, 2, R, w), bf16) for _, w in CHUNKS]
        + [pltpu.VMEM((rows_of(w), 128), f32) for _, w in CHUNKS]
        + [pltpu.VMEM((15, rows_of(w), 128), f32) for _, w in CHUNKS]
        + [pltpu.VMEM((rows_of(w), 128), f32) for _, w in CHUNKS]
        + [
            pltpu.VMEM((8, R, R), bf16),
            pltpu.VMEM((8, R, R), bf16),
            pltpu.VMEM((16, R, R), bf16),
            pltpu.VMEM((16, 2, R), f32),
            pltpu.VMEM((2, 7, 8, R), f32),
            pltpu.VMEM((2, 7, 8, R), f32),
            pltpu.VMEM((8, R, R), f32),
            pltpu.VMEM((8, R, 128), f32),
            pltpu.VMEM((8, 2, 56, 128), f32),
            pltpu.VMEM((2, 7, 56, 128), f32),
            pltpu.VMEM((2, 2, 7, 4, 128), f32),
            pltpu.VMEM((2, 2, 7, 4, 128), f32),
            sem((N, 8)),
            sem((2,)),
            sem((4,)),
            sem((N,)),
            sem((N,)),
            sem((2,)),
            sem((2,)),
            sem((2, 2)),
            sem((2, 2)),
        ],
        compiler_params=pltpu.CompilerParams(
            collective_id=0, has_side_effects=True, vmem_limit_bytes=52 * 1024 * 1024
        ),
    )(sp, op, sa, oa, se, oe, sr, orr)
    same, opposite = pl.pallas_call(
        hand_out,
        out_shape=[out, out],
        in_specs=[vmem, vmem],
        out_specs=[vmem, vmem],
        compiler_params=pltpu.CompilerParams(vmem_limit_bytes=1024 * 1024),
    )(same, opposite)
    return jnp.transpose(same, (1, 0, 2)), jnp.transpose(opposite, (1, 0, 2))


def solution(mesh):
    panels = P("aux", None, None, "pair")
    return jax.shard_map(
        body,
        mesh=mesh,
        in_specs=(panels, panels) + (P(),) * 6,
        out_specs=(P("pair", "aux", None), P("pair", "aux", None)),
        check_vma=False,
    )
```

```python
import jax
import jax.numpy as jnp
from jax import lax
from jax.experimental import pallas as pl
from jax.experimental.pallas import tpu as pltpu
from jax.sharding import PartitionSpec as P

f32 = jnp.float32
bf16 = jnp.bfloat16
MESH = pl.DeviceIdType.MESH

R = 112
CHUNKS = ((0, 1024), (1024, 1792), (2816, 2048), (4864, 1664), (6528, 960))
N = len(CHUNKS)
HELD = 3
LATE = 4
NT = (((1,), (1,)), ((), ()))


def tiles_of(width):
    return (width + 127) // 128


def rows_of(width):
    return (tiles_of(width) + 7) // 8 * 8


def kernel(
    sp, op, sa, oa, se, oe, sr, orr, out_s, out_o, *scratch
):
    pan, cps, crs, cs = (scratch[N * k : N * k + N] for k in range(4))
    (
        raw, tm, famp, fen, fadd, fmask, acc, tot, sb1, rb1, sb2, rb2,
        pan_sem, raw_sem, fin_sem, c_send, c_recv, s1_send, s1_recv, s2_send, s2_recv,
    ) = scratch[4 * N :]
    p = lax.axis_index("pair")
    a = lax.axis_index("aux")
    diagonal = p == a // 2

    raw_copies = [
        pltpu.make_async_copy(src.at[pl.ds(4 * a, 4)], raw.at[pl.ds(4 * s, 4)], raw_sem.at[s])
        for s, src in enumerate((sa, oa))
    ]
    for copy in raw_copies:
        copy.start()
    pan_copies = []
    for c, (start, width) in enumerate(CHUNKS):
        row = []
        for i in range(8):
            src = (sp if i < 4 else op).at[i % 4, :, :, pl.ds(start, width)]
            copy = pltpu.make_async_copy(src, pan[c].at[i], pan_sem.at[c, i])
            copy.start(priority=1)
            row.append(copy)
        pan_copies.append(row)
    fin_copies = []
    for s, (amp, en) in enumerate(((sa, se), (oa, oe))):
        fin_copies.append(
            pltpu.make_async_copy(amp.at[pl.ds(8 * p, 8)], famp.at[pl.ds(8 * s, 8)], fin_sem.at[s])
        )
        fin_copies.append(
            pltpu.make_async_copy(en.at[pl.ds(8 * p, 8)], fen.at[pl.ds(8 * s, 8)], fin_sem.at[2 + s])
        )
    for copy in fin_copies:
        copy.start()

    barrier = pltpu.get_barrier_semaphore()
    for k in range(1, 16):
        pl.semaphore_signal(
            barrier, inc=1, device_id=(p, lax.rem(a + k, 16)), device_id_type=MESH
        )
    for k in range(1, 8):
        pl.semaphore_signal(barrier, inc=1, device_id=(lax.rem(p + k, 8), a), device_id_type=MESH)
    own = lax.rem(a, 2)
    for k in range(2):

        @pl.when(jnp.logical_not(jnp.logical_and(diagonal, own == k)))
        def _():
            pl.semaphore_signal(
                barrier, inc=1, device_id=(a // 2, 2 * p + k), device_id_type=MESH
            )

    for copy in raw_copies:
        copy.wait()
    rows_i = lax.broadcasted_iota(jnp.int32, (R, R), 0)
    cols_i = lax.broadcasted_iota(jnp.int32, (R, R), 1)
    for i in range(8):
        rank = (sr if i < 4 else orr)[4 * a + i % 4]
        kept = jnp.logical_and(rows_i < rank, cols_i < rank)
        tm[i] = jnp.where(kept, raw[i].astype(f32), 0.0).astype(bf16)

    def mixed(c):
        width = CHUNKS[c][1]

        total = jnp.zeros((8, width), f32)
        for i in range(8):
            m = jnp.dot(tm[i], pan[c][i, 1], preferred_element_type=f32)
            prod = m * pan[c][i, 0].astype(f32)
            total = total + jnp.sum(prod.reshape(14, 8, width), axis=0)
        line = jnp.sum(total, axis=0, keepdims=True)
        for k in range(tiles_of(width)):
            part = min(128, width - 128 * k)
            cps[c][k : k + 1, 0:part] = line[:, 128 * k : 128 * k + part]

    def send_coupling(c):
        for k in range(1, 16):
            pltpu.make_async_remote_copy(
                src_ref=cps[c],
                dst_ref=crs[c].at[k - 1],
                send_sem=c_send.at[c],
                recv_sem=c_recv.at[c],
                device_id=(p, lax.rem(a + k, 16)),
                device_id_type=MESH,
            ).start()

    def take_coupling(c):
        pltpu.make_async_copy(crs[c], crs[c], c_recv.at[c]).wait()
        total = cps[c][...]
        for k in range(15):
            total = total + crs[c][k]
        cs[c][...] = total

    def exchange(c):
        for i in range(8):
            e = lax.dot_general(pan[c][i, 0], pan[c][i, 1], NT, preferred_element_type=f32)
            acc[i] = e if c == 0 else acc[i] + e

    def coulomb(c, i):
        width = CHUNKS[c][1]
        parts = []
        for t in range(tiles_of(width)):
            size = min(128, width - 128 * t)
            left = pan[c][i, 0, :, 128 * t : 128 * t + size].astype(f32)
            parts.append((left * cs[c][t : t + 1, 0:size]).astype(bf16))
        scaled = jnp.concatenate(parts, axis=1)
        return lax.dot_general(scaled, pan[c][i, 1], NT, preferred_element_type=f32)

    tot[...] = jnp.zeros_like(tot)
    tot[...] = jnp.zeros_like(tot)

    def prepare(c):
        cps[c][...] = jnp.zeros_like(cps[c])
        for i in range(8):
            pan_copies[c][i].wait()
        mixed(c)
        if c == 0:
            pl.semaphore_wait(barrier, 24 - diagonal.astype(jnp.int32))
        send_coupling(c)

    for c in range(N):
        prepare(c)
        if c < N - HELD:
            exchange(c)
    for c in range(N - HELD, N):
        exchange(c)

    for c in range(N - LATE):
        take_coupling(c)
        for i in range(8):
            acc[i] = acc[i] + coulomb(c, i)

    for c in range(N - LATE, N):
        take_coupling(c)
    for s in range(2):
        for j in range(4):
            i = 4 * s + j
            total = acc[i]
            for c in range(N - LATE, N):
                total = total + coulomb(c, i)
            tot[i, :, 0:R] = total
            for d in range(8):
                sb1[d, s, pl.ds(j, 14, stride=4), :] = tot[i, 14 * d : 14 * d + 14, :]
        for k in range(1, 8):
            d = lax.rem(p + k, 8)
            pltpu.make_async_remote_copy(
                src_ref=sb1.at[d, s],
                dst_ref=rb1.at[s, k - 1],
                send_sem=s1_send.at[s],
                recv_sem=s1_recv.at[s],
                device_id=(d, a),
                device_id_type=MESH,
            ).start()

    for copy in fin_copies:
        copy.wait()
    sel_r = lax.broadcasted_iota(jnp.int32, (16, R), 0)
    sel_c = lax.broadcasted_iota(jnp.int32, (16, R), 1)
    first = 7 * a
    chosen = jnp.logical_and(sel_c == first + sel_r, sel_r < 7)
    select = chosen.astype(f32).astype(bf16)
    pick = chosen[0:8].astype(f32)
    for k in range(16):
        rank = (sr if k < 8 else orr)[8 * p + k % 8]
        amp = jnp.dot(select, famp[k], preferred_element_type=f32)[0:8]
        first_gap = jnp.sum(pick * fen[k, 0:1, :], axis=1, keepdims=True)
        kept = jnp.logical_and(first + sel_r[0:8] < rank, sel_c[0:8] < rank).astype(f32)
        added = (first_gap + fen[k, 1:2, :]) * amp
        for r in range(7):
            fmask[k // 8, r, k % 8 : k % 8 + 1, :] = kept[r : r + 1]
            fadd[k // 8, r, k % 8 : k % 8 + 1, :] = added[r : r + 1]

    for s in range(2):
        pltpu.make_async_copy(rb1.at[s], rb1.at[s], s1_recv.at[s]).wait()
        total = sb1[p, s]
        for k in range(7):
            total = total + rb1[s, k]
        for r in range(14):
            sb2[r // 7, s, r % 7] = total[4 * r : 4 * r + 4]
        for q in range(2):
            mine = jnp.logical_and(diagonal, own == q)

            @pl.when(mine)
            def _():
                rb2[q, s] = sb2[q, s]

            @pl.when(jnp.logical_not(mine))
            def _():
                pltpu.make_async_remote_copy(
                    src_ref=sb2.at[q, s],
                    dst_ref=rb2.at[own, s],
                    send_sem=s2_send.at[q, s],
                    recv_sem=s2_recv.at[own, s],
                    device_id=(a // 2, 2 * p + q),
                    device_id_type=MESH,
                ).start()

    for s, out in enumerate((out_s, out_o)):
        for b in range(2):

            @pl.when(jnp.logical_not(jnp.logical_and(diagonal, own == b)))
            def _():
                pltpu.make_async_copy(rb2.at[b, s], rb2.at[b, s], s2_recv.at[b, s]).wait()
                pltpu.make_async_copy(rb2.at[b, s], rb2.at[b, s], s2_send.at[b, s]).wait()

        for r in range(7):
            value = jnp.concatenate([rb2[0, s, r, :, 0:R], rb2[1, s, r, :, 0:R]], axis=0)
            out[r] = (value + fadd[s, r]) * fmask[s, r]

    for c in range(N):
        pltpu.make_async_copy(crs[c], crs[c], c_send.at[c]).wait()
    for s in range(2):
        pltpu.make_async_copy(rb1.at[s], rb1.at[s], s1_send.at[s]).wait()


def hand_out(same, opposite, out_s, out_o, sem):
    copies = [
        pltpu.make_async_copy(src, dst, sem.at[k])
        for k, (src, dst) in enumerate(((same, out_s), (opposite, out_o)))
    ]
    for copy in copies:
        copy.start()
    for copy in copies:
        copy.wait()


def body(sp, op, sa, oa, se, oe, sr, orr):
    any_space = pl.BlockSpec(memory_space=pl.ANY)
    smem = pl.BlockSpec(memory_space=pltpu.SMEM)
    vmem = pl.BlockSpec(memory_space=pltpu.VMEM)
    out = jax.ShapeDtypeStruct((7, 8, R), f32)
    sem = pltpu.SemaphoreType.DMA
    sp, op, sa, oa, se, oe, sr, orr = (
        pltpu.with_memory_space_constraint(x, pltpu.HBM) for x in (sp, op, sa, oa, se, oe, sr, orr)
    )
    same, opposite = pl.pallas_call(
        kernel,
        out_shape=[out, out],
        in_specs=[any_space] * 6 + [smem] * 2,
        out_specs=[vmem, vmem],
        scratch_shapes=[pltpu.VMEM((8, 2, R, w), bf16) for _, w in CHUNKS]
        + [pltpu.VMEM((rows_of(w), 128), f32) for _, w in CHUNKS]
        + [pltpu.VMEM((15, rows_of(w), 128), f32) for _, w in CHUNKS]
        + [pltpu.VMEM((rows_of(w), 128), f32) for _, w in CHUNKS]
        + [
            pltpu.VMEM((8, R, R), bf16),
            pltpu.VMEM((8, R, R), bf16),
            pltpu.VMEM((16, R, R), bf16),
            pltpu.VMEM((16, 2, R), f32),
            pltpu.VMEM((2, 7, 8, R), f32),
            pltpu.VMEM((2, 7, 8, R), f32),
            pltpu.VMEM((8, R, R), f32),
            pltpu.VMEM((8, R, 128), f32),
            pltpu.VMEM((8, 2, 56, 128), f32),
            pltpu.VMEM((2, 7, 56, 128), f32),
            pltpu.VMEM((2, 2, 7, 4, 128), f32),
            pltpu.VMEM((2, 2, 7, 4, 128), f32),
            sem((N, 8)),
            sem((2,)),
            sem((4,)),
            sem((N,)),
            sem((N,)),
            sem((2,)),
            sem((2,)),
            sem((2, 2)),
            sem((2, 2)),
        ],
        compiler_params=pltpu.CompilerParams(
            collective_id=0, has_side_effects=True, vmem_limit_bytes=52 * 1024 * 1024
        ),
    )(sp, op, sa, oa, se, oe, sr, orr)
    same, opposite = pl.pallas_call(
        hand_out,
        out_shape=[out, out],
        in_specs=[vmem, vmem],
        out_specs=[any_space, any_space],
        scratch_shapes=[sem((2,))],
        compiler_params=pltpu.CompilerParams(vmem_limit_bytes=1024 * 1024),
    )(same, opposite)
    return jnp.transpose(same, (1, 0, 2)), jnp.transpose(opposite, (1, 0, 2))


def solution(mesh):
    panels = P("aux", None, None, "pair")
    return jax.shard_map(
        body,
        mesh=mesh,
        in_specs=(panels, panels) + (P(),) * 6,
        out_specs=(P("pair", "aux", None), P("pair", "aux", None)),
        check_vma=False,
    )
```
